32 devices in a mesh: expert: 2 (over x), batch: 4 (over z), seq: 4 (over y, core).
Axes of the slice: x: 2, y: 2, z: 4, core: 2. Of those that a mesh axis runs over, the one named last changes fastest.
Arguments:
- queries: bfloat16 [2, 4, 2, 384, 4096], P('expert', 'batch', None, 'seq'), may hold values from -36 to 36
- keys: bfloat16 [2, 4, 2, 384, 4096], P('expert', 'batch', None, 'seq'), may hold values from -21 to 21
- values: bfloat16 [2, 4, 2, 384, 4096], P('expert', 'batch', None, 'seq'), may hold values from -6 to 6
- latents: bfloat16 [2, 4, 384, 4096], P('expert', 'batch', 'seq'), may hold values from -6 to 6
- gain: bfloat16 [2, 4096], P('expert'), may hold values from 0.099609375 to 1.8984375
- steps_table: int32 [2, 4], P('expert', 'batch'), may hold values from 0 to 38
- flags: int32 [4], P('batch'), may hold values 0 or 1
Outputs:
- denoised: bfloat16 [2, 4, 384, 4096], P('expert', 'batch', 'seq')
- next_latents: bfloat16 [2, 4, 384, 4096], P('expert', 'batch', 'seq')
The draws below stay inside these ranges and needn't reach their ends.
All inputs are finite; a program needn't handle non-finite values. No bound on the sum of `flags` on one device may be relied on, other than what follows from the above.
Results may differ from the reference program's by a relative error of at most 0.006.
Values may be sent and summed in bfloat16 or wider, within the bound.
A program may use at most 64 MiB of HBM per device.

```python
import jax
import jax.numpy as jnp
from jax import lax

HEADS = 32
HDIM = 128
STEPS = 40
BOUNDARY = 15
BATCH = 4
SEQ = 384
WIDTH = 4096


def paired_draw(key):
    base = jax.random.fold_in(key, 7)
    query_key, key_key = jax.random.split(base, 2)
    shape = (2, BATCH, 2, SEQ, HEADS * HDIM)
    query_part = jnp.clip(jax.random.normal(query_key, shape, jnp.float32), -5.0, 5.0)
    key_part = jnp.clip(jax.random.normal(key_key, shape, jnp.float32), -5.0, 5.0)
    return (query_part, key_part)


def draw_queries(key, part):
    return paired_draw(key)[0].astype(jnp.bfloat16)


def draw_keys(key, part):
    return paired_draw(key)[1].astype(jnp.bfloat16)


def draw_steps_table(key, part):
    base = jax.random.fold_in(key, 11)
    high_key, low_key, high_pick, low_pick = jax.random.split(base, 4)
    high_steps = jax.random.randint(high_key, (BATCH,), 0, BOUNDARY)
    low_steps = jax.random.randint(low_key, (BATCH,), BOUNDARY, STEPS - 1)
    places = jnp.arange(BATCH, dtype=jnp.int32)
    high_spot = jax.random.randint(high_pick, (), 0, BATCH)
    low_spot = jax.random.randint(low_pick, (), 0, BATCH)
    high_steps = jnp.where(places == high_spot, 0, high_steps)
    low_steps = jnp.where(places == low_spot, STEPS - 2, low_steps)
    return jnp.stack([high_steps, low_steps], axis=0).astype(jnp.int32)


def touch_ends(values, stream_key, low, largest):
    longest = values.shape.index(max(values.shape))
    spots = []
    for shift in (0, 1):
        where = [jax.random.randint(jax.random.fold_in(stream_key, axis), (), 0, length) for axis, length in enumerate(values.shape)]
        where[longest] = (where[longest] + shift) % values.shape[longest]
        spots.append(tuple(where))
    return values.at[spots[0]].set(low).at[spots[1]].set(largest)


def levels(stream_key, extent, shards, least, high):
    level, own = 1.0, jax.random.fold_in(stream_key, 6)
    for axis_at, parts in shards:
        heights = jnp.exp(jax.random.uniform(jax.random.fold_in(own, axis_at), (parts,), jnp.float32, least / len(shards), high / len(shards)))
        level = level * jnp.repeat(heights, extent[axis_at] // parts).reshape([-1 if axis == axis_at else 1 for axis in range(len(extent))])
    return level


def gaussian(rng, extent, scale, most, cuts=(), kind=jnp.bfloat16):
    result = scale * jax.random.normal(rng, extent, jnp.float32)
    if cuts:
        result = result * levels(rng, extent, cuts, -0.22, 0.18)
    return jnp.clip(result, -most, most).astype(kind)


def setup_inputs(seed: int = 0) -> dict:
    seeds = jax.random.split(jax.random.key(seed), 8)
    queries = draw_queries(jax.random.fold_in(seeds[7], 71), 0)
    keys = draw_keys(jax.random.fold_in(seeds[7], 71), 0)
    values = gaussian(seeds[2], (2, BATCH, 2, SEQ, WIDTH), 1.0, 6.0, ((0, 2), (1, 4), (3, 4)))
    latents = gaussian(seeds[3], (2, BATCH, SEQ, WIDTH), 1.0, 6.0, ((0, 2), (1, 4), (2, 4)))
    gain = jnp.clip(1.0 + 0.18 * jax.random.normal(seeds[4], (2, WIDTH), jnp.float32), 0.099609375, 1.8984375).astype(jnp.bfloat16)
    steps_table = draw_steps_table(jax.random.fold_in(seeds[7], 71), 0)
    flags = touch_ends((jax.random.randint(seeds[6], (BATCH,), 0, 2) < 1).astype(jnp.int32), jax.random.fold_in(seeds[6], 1), 0, 1)
    return dict(queries=queries, keys=keys, values=values, latents=latents, gain=gain, steps_table=steps_table, flags=flags)


GUIDANCE = 3.5
flow_shift = 5.0

def sigma_of(step):
    level = 1.0 - step.astype(jnp.float32) / STEPS
    return flow_shift * level / (1.0 + (flow_shift - 1.0) * level)

def attend_head(query, key_rows, value_rows):
    scores = jnp.dot(query, key_rows.T, preferred_element_type=jnp.float32) * HDIM ** (-0.5)
    weights = jax.nn.softmax(scores, axis=-1).astype(jnp.bfloat16)
    return jnp.dot(weights, value_rows, preferred_element_type=jnp.float32).astype(jnp.bfloat16)

def combine(cond, uncond):
    base = uncond.astype(jnp.float32)
    return (base + GUIDANCE * (cond.astype(jnp.float32) - base)).astype(jnp.bfloat16)

def reference(queries, keys, values, latents, gain, steps_table, flags):
    groups, clips, branches, length, width = queries.shape

    def heads_first(array):
        shaped = array.reshape(groups * clips * branches, length, HEADS, HDIM)
        return shaped.transpose(0, 2, 1, 3).reshape(-1, length, HDIM)
    outcome = lax.map(lambda triple: attend_head(*triple), (heads_first(queries), heads_first(keys), heads_first(values)))
    attended = outcome.reshape(groups, clips, branches, HEADS, length, HDIM)
    attended = attended.transpose(0, 1, 2, 4, 3, 5).reshape(groups, clips, branches, length, width)
    guided = combine(attended[:, :, 0], attended[:, :, 1]).astype(jnp.float32)
    scale = lax.rsqrt(lax.optimization_barrier(jnp.mean(guided * guided, axis=-1, keepdims=True)) + 1e-06)
    velocity = guided * scale * gain.astype(jnp.float32)[:, None, None, :]
    sigma_now = sigma_of(steps_table)[:, :, None, None]
    sigma_next = sigma_of(steps_table + 1)[:, :, None, None]
    current = latents.astype(jnp.float32)
    denoised = (current - sigma_now * velocity).astype(jnp.bfloat16)
    moved = (current + (sigma_next - sigma_now) * velocity).astype(jnp.bfloat16)
    crossing = (flags == 1)[None, :, None, None]
    next_latents = jnp.where(crossing, moved[::-1], moved)
    return (denoised, next_latents)
```

```python
import functools

import jax
import jax.numpy as jnp
from jax import lax
from jax.experimental import pallas as pl
from jax.experimental.pallas import tpu as pltpu
from jax.sharding import PartitionSpec as P

HDIM = 128
STEPS = 40


GUIDANCE = 3.5
flow_shift = 5.0


def from_partner(block, axis, bit):
    count = lax.axis_size(axis)
    route = []
    for low in range(count):
        high = low | 1 << bit
        if high != low and high < count:
            route += [(low, high), (high, low)]
    return lax.ppermute(block, axis, route)


def sigma_of(step):
    level = 1.0 - step.astype(jnp.float32) / STEPS
    return flow_shift * level / (1.0 + (flow_shift - 1.0) * level)


def combine(cond, uncond):
    base = uncond.astype(jnp.float32)
    return (base + GUIDANCE * (cond.astype(jnp.float32) - base)).astype(jnp.bfloat16)


def attend(stacked):
    query_heads, key_heads, value_heads = stacked
    items, length, width_dev = query_heads.shape
    heads_dev = width_dev // HDIM
    block = 512 if length % 512 == 0 else length
    key_rows = key_heads.reshape(items, length, heads_dev, HDIM)
    value_rows = value_heads.reshape(items, length, heads_dev, HDIM)
    query_blocks = query_heads.reshape(items, length // block, block, heads_dev, HDIM).transpose(
        1, 0, 2, 3, 4
    )

    def one_block(query_part):
        scores = jnp.einsum(
            "nqhd,nkhd->nhqk", query_part, key_rows, preferred_element_type=jnp.float32
        ) * HDIM ** (-0.5)
        weights = jax.nn.softmax(scores, axis=-1).astype(jnp.bfloat16)
        return jnp.einsum(
            "nhqk,nkhd->nqhd", weights, value_rows, preferred_element_type=jnp.float32
        ).astype(jnp.bfloat16)

    result = lax.map(one_block, query_blocks)
    return result.transpose(1, 0, 2, 3, 4).reshape(items, length, width_dev)


def exchange_heads(queries, keys, values, latents, gain, steps_table, flags):
    attended = attend(
        (
            lax.all_to_all(queries[0, 0], "seq", split_axis=2, concat_axis=1, tiled=True),
            lax.all_to_all(keys[0, 0], "seq", split_axis=2, concat_axis=1, tiled=True),
            lax.all_to_all(values[0, 0], "seq", split_axis=2, concat_axis=1, tiled=True),
        )
    )
    guided = lax.all_to_all(
        combine(attended[0], attended[1]), "seq", split_axis=0, concat_axis=1, tiled=True
    )
    guided_f32 = guided.astype(jnp.float32)
    scale = lax.rsqrt(jnp.mean(guided_f32 * guided_f32, axis=-1, keepdims=True) + 1e-06)
    velocity = guided_f32 * scale * gain[0].astype(jnp.float32)[None, :]
    step_now = steps_table[0, 0]
    sigma_now = sigma_of(step_now)
    sigma_next = sigma_of(step_now + 1)
    current = latents[0, 0].astype(jnp.float32)
    denoised = (current - sigma_now * velocity).astype(jnp.bfloat16)
    moved = (current + (sigma_next - sigma_now) * velocity).astype(jnp.bfloat16)
    partner = from_partner(moved, "expert", 0)
    next_latents = jnp.where(flags[0] == 1, partner, moved)
    return (denoised[None, None], next_latents[None, None])


MESH = pl.DeviceIdType.MESH
HEADS_AT_ONCE = 4
EARLY = 3
TILE = 8
LOG2E = 1.4426950408889634


def partial_attention(query, key_rows, value_rows):
    scores = lax.dot_general(
        query, key_rows, (((1,), (1,)), ((), ())), preferred_element_type=jnp.float32
    )
    top = jnp.max(scores, axis=-1, keepdims=True)
    powers = jnp.exp2((scores - top) * (HDIM ** (-0.5) * LOG2E))
    total = jnp.sum(powers, axis=-1, keepdims=True)
    part = jnp.dot(powers.astype(jnp.bfloat16), value_rows, preferred_element_type=jnp.float32)
    return part, total, top * (HDIM ** (-0.5) * LOG2E) + jnp.log2(total)


def share(mine, other):
    return 1.0 / (1.0 + jnp.exp2(other - mine))


def pack(stat, spot, packed):
    lane = lax.broadcasted_iota(jnp.int32, packed.shape, 1)
    for at in range(stat.shape[0] // TILE):
        here = stat[at * TILE : (at + 1) * TILE]
        packed = jnp.where(lane == at * TILE + spot, here, packed)
    return packed


def unpack(packed, spot, rows):
    return jnp.concatenate(
        [packed[:, at * TILE + spot : at * TILE + spot + 1] for at in range(rows // TILE)], axis=0
    )


def pair_kernel(
    queries, keys, values, latents, gain, steps, flags,
    denoised, next_latents,
    q_own, q_far, k_all, v_all, part_own, part_far, part_back, guided, guided_peer,
    now, now_peer, lse_own, lse_peer, lse_far, lse_back, squares, squares_peer,
    gain_now, gain_move, gain_peer,
    load_sems, kv_sems, q_sems, lse_sems, back_sems, stat_sems, cross_sems, ahead_sems,
):
    seq = lax.axis_index("seq")
    size = lax.axis_size("seq")
    beside = {"seq": seq + 1 - 2 * lax.rem(seq, 2)}
    across = {"seq": lax.rem(seq + size // 2, size)}
    other = {"expert": 1 - lax.axis_index("expert")}
    branches, rows, width = queries.shape
    group = HEADS_AT_ONCE * HDIM
    groups = width // group

    own_keys = pl.ds(0, rows)
    peer_keys = pl.ds(rows, rows)
    loads = [
        pltpu.make_async_copy(keys, k_all.at[:, own_keys], load_sems.at[0]),
        pltpu.make_async_copy(queries, q_own, load_sems.at[1]),
        pltpu.make_async_copy(values, v_all.at[:, own_keys], load_sems.at[2]),
        pltpu.make_async_copy(latents, now, load_sems.at[3]),
    ]
    for load in loads:
        load.start()

    barrier = pltpu.get_barrier_semaphore()
    for peer in (beside, across, other):
        pl.semaphore_signal(barrier, inc=1, device_id=peer, device_id_type=MESH)
    pl.semaphore_wait(barrier, 3)

    def remote(source, target, sems, index, peer):
        return pltpu.make_async_remote_copy(
            src_ref=source, dst_ref=target, send_sem=sems.at[0, index],
            recv_sem=sems.at[1, index], device_id=peer, device_id_type=MESH,
        )

    def span(at):
        return pl.ds(pl.multiple_of(at * group, group), group)

    def head_span(at, extra):
        return pl.ds(pl.multiple_of(at * group + extra * HDIM, HDIM), HDIM)

    def q_send(at):
        cols = span(at)
        return remote(queries.at[:, :, cols], q_far.at[:, :, cols], q_sems, at, across)

    def kv_sends(at):
        cols = span(at)
        return (
            remote(keys.at[:, :, cols], k_all.at[:, peer_keys, cols], kv_sems, 2 * at, beside),
            remote(values.at[:, :, cols], v_all.at[:, peer_keys, cols], kv_sems, 2 * at + 1, beside),
        )

    def lse_send(at):
        return remote(lse_own.at[at], lse_peer.at[at], lse_sems, at, across)

    def back_sends(at):
        cols = span(at)
        return (
            remote(lse_far.at[at], lse_back.at[at], stat_sems, at, across),
            remote(part_far.at[:, cols], part_back.at[:, cols], back_sems, at, across),
        )

    def cross_send(at):
        cols = span(at)
        return remote(guided.at[:, cols], guided_peer.at[:, cols], cross_sems, at, other)

    for at in range(min(EARLY, groups)):
        q_send(at).start()

    def start_kv(at, carry):
        for send in kv_sends(at):
            send.start()
        return carry

    lax.fori_loop(0, groups, start_kv, 0)
    ahead = [
        remote(latents, now_peer, ahead_sems, 0, other),
        remote(gain_move, gain_peer, ahead_sems, 1, other),
    ]
    ahead[0].start()

    step = jnp.full((1, HDIM), steps[0, 0], jnp.int32)
    sigma_now = sigma_of(step)[:, :1]
    sigma_next = sigma_of(step + 1)[:, :1]
    row = gain[...].astype(jnp.float32)
    gain_now[...] = sigma_now * row
    gain_move[...] = (sigma_next - sigma_now) * row
    squares[...] = jnp.zeros_like(squares)
    squares_peer[...] = jnp.zeros_like(squares_peer)

    for load in loads:
        load.wait()

    def own_group(at, carry):
        for send in kv_sends(at):
            send.wait_recv()
        lse = jnp.zeros((TILE, HDIM), jnp.float32)
        for extra in range(HEADS_AT_ONCE):
            cols = head_span(at, extra)
            for branch in range(branches):
                part, total, stat = partial_attention(
                    q_own[branch, :, cols], k_all[branch, :, cols], v_all[branch, :, cols]
                )
                part_own[branch, :, cols] = part / total
                lse = pack(stat, extra * branches + branch, lse)
        lse_own[at] = lse
        lse_send(at).start()

        @pl.when(at + EARLY < groups)
        def _():
            q_send(at + EARLY).start()

        return carry

    lax.fori_loop(0, groups, own_group, 0)
    ahead[1].start()

    def far_group(at, carry):
        lse_send(at).wait_recv()
        q_send(at).wait_recv()
        theirs = lse_peer[at]
        lse = jnp.zeros((TILE, HDIM), jnp.float32)
        for extra in range(HEADS_AT_ONCE):
            cols = head_span(at, extra)
            terms = []
            for branch, factor in ((0, GUIDANCE), (1, 1.0 - GUIDANCE)):
                part, total, stat = partial_attention(
                    q_far[branch, :, cols], k_all[branch, :, cols], v_all[branch, :, cols]
                )
                spot = extra * branches + branch
                lse = pack(stat, spot, lse)
                terms.append(part * (factor * share(stat, unpack(theirs, spot, rows)) / total))
            part_far[:, cols] = (terms[0] + terms[1]).astype(jnp.bfloat16)
        lse_far[at] = lse
        for send in back_sends(at):
            send.start()
        return carry

    lax.fori_loop(0, groups, far_group, 0)

    def add_squares(target, values_here):
        target[...] += values_here * values_here

    def finish_group(at, carry):
        for send in back_sends(at):
            send.wait_recv()
        weight = share(lse_own[at], lse_back[at])
        for extra in range(HEADS_AT_ONCE):
            cols = head_span(at, extra)
            spot = extra * branches
            value = (
                GUIDANCE * unpack(weight, spot, rows) * part_own[0, :, cols]
                + (1.0 - GUIDANCE) * unpack(weight, spot + 1, rows) * part_own[1, :, cols]
                + part_back[:, cols].astype(jnp.float32)
            ).astype(jnp.bfloat16)
            guided[:, cols] = value
            add_squares(squares, value.astype(jnp.float32))
        cross_send(at).start()
        return carry

    lax.fori_loop(0, groups, finish_group, 0)

    scale = lax.rsqrt(jnp.sum(squares[...], axis=-1, keepdims=True) / width + 1e-06)

    def denoise_group(at, carry):
        for extra in range(HEADS_AT_ONCE):
            cols = head_span(at, extra)
            unit = guided[:, cols].astype(jnp.float32) * scale
            denoised[:, cols] = (
                now[:, cols].astype(jnp.float32) - gain_now[:, cols] * unit
            ).astype(jnp.bfloat16)
        return carry

    lax.fori_loop(0, groups, denoise_group, 0)

    def peer_squares(at, carry):
        cross_send(at).wait_recv()
        for extra in range(HEADS_AT_ONCE):
            add_squares(squares_peer, guided_peer[:, head_span(at, extra)].astype(jnp.float32))
        return carry

    lax.fori_loop(0, groups, peer_squares, 0)
    for send in ahead:
        send.wait_recv()
    scale_peer = lax.rsqrt(jnp.sum(squares_peer[...], axis=-1, keepdims=True) / width + 1e-06)
    trade = jnp.full((rows, HDIM), flags[0], jnp.int32) == 1

    def move_group(at, carry):
        for extra in range(HEADS_AT_ONCE):
            cols = head_span(at, extra)
            mine = now[:, cols].astype(jnp.float32) + gain_move[:, cols] * (
                guided[:, cols].astype(jnp.float32) * scale
            )
            theirs = now_peer[:, cols].astype(jnp.float32) + gain_peer[:, cols] * (
                guided_peer[:, cols].astype(jnp.float32) * scale_peer
            )
            next_latents[:, cols] = jnp.where(trade, theirs, mine).astype(jnp.bfloat16)
        return carry

    lax.fori_loop(0, groups, move_group, 0)

    def drain(at, carry):
        for send in (q_send(at), lse_send(at), cross_send(at)) + kv_sends(at) + back_sends(at):
            send.wait_send()
        return carry

    lax.fori_loop(0, groups, drain, 0)
    for send in ahead:
        send.wait_send()


def exchange_queries(queries, keys, values, latents, gain, steps_table, flags):
    branches, rows, width = queries.shape[2:]
    groups = width // (HEADS_AT_ONCE * HDIM)
    whole = jax.ShapeDtypeStruct((rows, width), jnp.bfloat16)
    hbm = pl.BlockSpec(memory_space=pltpu.HBM)
    vmem = pl.BlockSpec(memory_space=pltpu.VMEM)
    smem = pl.BlockSpec(memory_space=pltpu.SMEM)
    low = functools.partial(pltpu.VMEM, dtype=jnp.bfloat16)
    high = functools.partial(pltpu.VMEM, dtype=jnp.float32)
    dma = pltpu.SemaphoreType.DMA
    stats = high((groups, TILE, HDIM))
    denoised, next_latents = pl.pallas_call(
        pair_kernel,
        out_shape=(whole, whole),
        in_specs=[hbm] * 4 + [vmem, smem, smem],
        out_specs=(vmem, vmem),
        scratch_shapes=[
            low((branches, rows, width)),
            low((branches, rows, width)),
            low((branches, 2 * rows, width)),
            low((branches, 2 * rows, width)),
            high((branches, rows, width)),
            low((rows, width)),
            low((rows, width)),
            low((rows, width)),
            low((rows, width)),
            low((rows, width)),
            low((rows, width)),
            stats,
            stats,
            stats,
            stats,
            high((rows, HDIM)),
            high((rows, HDIM)),
            high((1, width)),
            high((1, width)),
            high((1, width)),
            dma((4,)),
            dma((2, 2 * groups)),
            dma((2, groups)),
            dma((2, groups)),
            dma((2, groups)),
            dma((2, groups)),
            dma((2, groups)),
            dma((2, 2)),
        ],
        compiler_params=pltpu.CompilerParams(collective_id=0, has_side_effects=True),
    )(queries[0, 0], keys[0, 0], values[0, 0], latents[0, 0], gain, steps_table, flags)
    return (denoised[None, None], next_latents[None, None])


def per_device(*blocks):
    branches, rows, width = blocks[0].shape[2:]
    paired = (
        lax.axis_size("seq") == 2 * 2
        and lax.axis_size("expert") == 2
        and branches == 2
        and rows % (2 * TILE) == 0
        and rows // TILE * HEADS_AT_ONCE * branches <= HDIM
        and HEADS_AT_ONCE * branches <= TILE
        and width % (HEADS_AT_ONCE * HDIM) == 0
    )
    return (exchange_queries if paired else exchange_heads)(*blocks)


def solution(mesh):
    placed = (
        P("expert", "batch", None, "seq", None),
        P("expert", "batch", None, "seq", None),
        P("expert", "batch", None, "seq", None),
        P("expert", "batch", "seq", None),
        P("expert", None),
        P("expert", "batch"),
        P("batch"),
    )
    return jax.shard_map(
        per_device,
        mesh=mesh,
        in_specs=placed,
        out_specs=(P("expert", "batch", "seq", None), P("expert", "batch", "seq", None)),
        check_vma=False,
    )
```

```python
import functools

import jax
import jax.numpy as jnp
from jax import lax
from jax.experimental import pallas as pl
from jax.experimental.pallas import tpu as pltpu
from jax.sharding import PartitionSpec as P

HDIM = 128
STEPS = 40


GUIDANCE = 3.5
flow_shift = 5.0


def from_partner(block, axis, bit):
    count = lax.axis_size(axis)
    route = []
    for low in range(count):
        high = low | 1 << bit
        if high != low and high < count:
            route += [(low, high), (high, low)]
    return lax.ppermute(block, axis, route)


def sigma_of(step):
    level = 1.0 - step.astype(jnp.float32) / STEPS
    return flow_shift * level / (1.0 + (flow_shift - 1.0) * level)


def combine(cond, uncond):
    base = uncond.astype(jnp.float32)
    return (base + GUIDANCE * (cond.astype(jnp.float32) - base)).astype(jnp.bfloat16)


def attend(stacked):
    query_heads, key_heads, value_heads = stacked
    items, length, width_dev = query_heads.shape
    heads_dev = width_dev // HDIM
    block = 512 if length % 512 == 0 else length
    key_rows = key_heads.reshape(items, length, heads_dev, HDIM)
    value_rows = value_heads.reshape(items, length, heads_dev, HDIM)
    query_blocks = query_heads.reshape(items, length // block, block, heads_dev, HDIM).transpose(
        1, 0, 2, 3, 4
    )

    def one_block(query_part):
        scores = jnp.einsum(
            "nqhd,nkhd->nhqk", query_part, key_rows, preferred_element_type=jnp.float32
        ) * HDIM ** (-0.5)
        weights = jax.nn.softmax(scores, axis=-1).astype(jnp.bfloat16)
        return jnp.einsum(
            "nhqk,nkhd->nqhd", weights, value_rows, preferred_element_type=jnp.float32
        ).astype(jnp.bfloat16)

    result = lax.map(one_block, query_blocks)
    return result.transpose(1, 0, 2, 3, 4).reshape(items, length, width_dev)


def exchange_heads(queries, keys, values, latents, gain, steps_table, flags):
    attended = attend(
        (
            lax.all_to_all(queries[0, 0], "seq", split_axis=2, concat_axis=1, tiled=True),
            lax.all_to_all(keys[0, 0], "seq", split_axis=2, concat_axis=1, tiled=True),
            lax.all_to_all(values[0, 0], "seq", split_axis=2, concat_axis=1, tiled=True),
        )
    )
    guided = lax.all_to_all(
        combine(attended[0], attended[1]), "seq", split_axis=0, concat_axis=1, tiled=True
    )
    guided_f32 = guided.astype(jnp.float32)
    scale = lax.rsqrt(jnp.mean(guided_f32 * guided_f32, axis=-1, keepdims=True) + 1e-06)
    velocity = guided_f32 * scale * gain[0].astype(jnp.float32)[None, :]
    step_now = steps_table[0, 0]
    sigma_now = sigma_of(step_now)
    sigma_next = sigma_of(step_now + 1)
    current = latents[0, 0].astype(jnp.float32)
    denoised = (current - sigma_now * velocity).astype(jnp.bfloat16)
    moved = (current + (sigma_next - sigma_now) * velocity).astype(jnp.bfloat16)
    partner = from_partner(moved, "expert", 0)
    next_latents = jnp.where(flags[0] == 1, partner, moved)
    return (denoised[None, None], next_latents[None, None])


MESH = pl.DeviceIdType.MESH
HEADS_AT_ONCE = 4
EARLY = 3
LAG = 2
TILE = 8
LOG2E = 1.4426950408889634


def partial_attentions(queries, key_blocks, value_blocks):
    scores = [
        lax.dot_general(query, rows, (((1,), (1,)), ((), ())), preferred_element_type=jnp.float32)
        for query, rows in zip(queries, key_blocks)
    ]
    tops = [jnp.max(score, axis=-1, keepdims=True) for score in scores]
    powers = [
        jnp.exp2((score - top) * (HDIM ** (-0.5) * LOG2E)).astype(jnp.bfloat16)
        for score, top in zip(scores, tops)
    ]
    ones = jnp.ones_like(value_blocks[0])
    sums = [
        jnp.dot(
            power, jnp.concatenate([rows, ones], axis=1), preferred_element_type=jnp.float32
        )
        for power, rows in zip(powers, value_blocks)
    ]
    parts = [both[:, :HDIM] for both in sums]
    totals = [both[:, HDIM:] for both in sums]
    stats = [
        top * (HDIM ** (-0.5) * LOG2E) + jnp.log2(total[:, :1]) for top, total in zip(tops, totals)
    ]
    return parts, totals, stats


def share(mine, other):
    return 1.0 / (1.0 + jnp.exp2(other - mine))


def pack(stat, spot, packed):
    lane = lax.broadcasted_iota(jnp.int32, packed.shape, 1)
    for at in range(stat.shape[0] // TILE):
        here = stat[at * TILE : (at + 1) * TILE]
        packed = jnp.where(lane == at * TILE + spot, here, packed)
    return packed


def unpack(packed, spot, rows):
    return jnp.concatenate(
        [packed[:, at * TILE + spot : at * TILE + spot + 1] for at in range(rows // TILE)], axis=0
    )


def pair_kernel(
    queries, keys, values, latents, gain_in, steps_in, flags_in,
    denoised, lifted, base, scale_out,
    q_own, q_far, k_all, v_all, part_own, part_far, part_back, guided, guided_peer,
    now, now_peer, lse_own, lse_peer, lse_far, lse_back, squares, squares_peer,
    gain, steps, flags, gain_now, gain_move, gain_peer, gain_next,
    load_sems, kv_sems, q_sems, lse_sems, back_sems, stat_sems, cross_sems, ahead_sems, ready,
):
    seq = lax.axis_index("seq")
    size = lax.axis_size("seq")
    side = lax.rem(seq, 2)
    beside = {"seq": seq + 1 - 2 * side}
    across = {"seq": lax.rem(seq + size // 2, size)}
    other = {"expert": 1 - lax.axis_index("expert")}
    branches, rows, width = queries.shape
    group = HEADS_AT_ONCE * HDIM
    groups = width // group
    last = groups - 1

    def signal(sem, peer):
        pl.semaphore_signal(sem, inc=1, device_id=peer, device_id_type=MESH)

    barrier = pltpu.get_barrier_semaphore()
    signal(barrier, across)

    @pl.when(side == 0)
    def _():
        signal(barrier, other)
        signal(barrier, beside)

    own_keys = pl.ds(0, rows)
    peer_keys = pl.ds(rows, rows)
    loads = [
        pltpu.make_async_copy(steps_in, steps, load_sems.at[0]),
        pltpu.make_async_copy(flags_in, flags, load_sems.at[1]),
        pltpu.make_async_copy(gain_in, gain, load_sems.at[2]),
        pltpu.make_async_copy(queries, q_own, load_sems.at[3]),
        pltpu.make_async_copy(keys, k_all.at[:, own_keys], load_sems.at[4]),
        pltpu.make_async_copy(values, v_all.at[:, own_keys], load_sems.at[5]),
        pltpu.make_async_copy(latents, now, load_sems.at[6]),
    ]
    for load in loads:
        load.start()
    pl.semaphore_wait(barrier, 2)

    def remote(source, target, sems, index, peer):
        return pltpu.make_async_remote_copy(
            src_ref=source, dst_ref=target, send_sem=sems.at[0, index],
            recv_sem=sems.at[1, index], device_id=peer, device_id_type=MESH,
        )

    def span(at):
        return pl.ds(pl.multiple_of(at * group, group), group)

    def head_span(at, extra):
        return pl.ds(pl.multiple_of(at * group + extra * HDIM, HDIM), HDIM)

    def q_send(at):
        cols = span(at)
        return remote(queries.at[:, :, cols], q_far.at[:, :, cols], q_sems, at, across)

    def kv_sends(at):
        cols = span(at)
        return (
            remote(keys.at[:, :, cols], k_all.at[:, peer_keys, cols], kv_sems, 2 * at, beside),
            remote(values.at[:, :, cols], v_all.at[:, peer_keys, cols], kv_sems, 2 * at + 1, beside),
        )

    def lse_send(at):
        return remote(lse_own.at[at], lse_peer.at[at], lse_sems, at, across)

    def stat_send(at):
        return remote(lse_far.at[at], lse_back.at[at], stat_sems, at, across)

    def back_send(cols, piece):
        return remote(part_far.at[:, cols], part_back.at[:, cols], back_sems, piece, across)

    def cross_send(cols, piece):
        return remote(guided.at[:, cols], guided_peer.at[:, cols], cross_sems, piece, other)

    endings = [(head_span(last, extra), last + extra) for extra in range(HEADS_AT_ONCE)]

    for at in range(min(EARLY, groups)):
        q_send(at).start()

    def start_kv():
        def step(at, carry):
            for send in kv_sends(at):
                send.start()
            return carry

        lax.fori_loop(0, groups, step, 0)

    ahead = [
        remote(latents, now_peer, ahead_sems, 0, other),
        remote(gain_move, gain_peer, ahead_sems, 1, other),
    ]

    @pl.when(side == 0)
    def _():
        pl.semaphore_wait(ready.at[0], 1)
        signal(ready.at[1], other)

    @pl.when(side == 1)
    def _():
        signal(ready.at[0], beside)

    start_kv()

    for load in loads[:3]:
        load.wait()
    step = jnp.broadcast_to(steps[...], (1, HDIM))
    sigma_now = sigma_of(step)[:, :1]
    sigma_next = sigma_of(step + 1)[:, :1]
    row = gain[...].astype(jnp.float32)
    gain_now[...] = sigma_now * row
    gain_move[...] = (sigma_next - sigma_now) * row
    squares[...] = jnp.zeros_like(squares)
    squares_peer[...] = jnp.zeros_like(squares_peer)
    for load in loads[3:]:
        load.wait()

    def units_of(at):
        return [
            (branch, head_span(at, extra), extra * branches + branch)
            for extra in range(HEADS_AT_ONCE)
            for branch in range(branches)
        ]

    def own_group(at, carry):
        for send in kv_sends(at):
            send.wait_recv()
        units = units_of(at)
        parts, totals, stats = partial_attentions(
            [q_own[branch, :, cols] for branch, cols, _ in units],
            [k_all[branch, :, cols] for branch, cols, _ in units],
            [v_all[branch, :, cols] for branch, cols, _ in units],
        )
        lse = jnp.zeros((TILE, HDIM), jnp.float32)
        for (branch, cols, spot), part, total, stat in zip(units, parts, totals, stats):
            part_own[branch, :, cols] = part / total
            lse = pack(stat, spot, lse)
        lse_own[at] = lse
        lse_send(at).start()

        @pl.when(at + EARLY < groups)
        def _():
            q_send(at + EARLY).start()

        return carry

    lax.fori_loop(0, groups, own_group, 0)

    @pl.when(side == 0)
    def _():
        pl.semaphore_wait(ready.at[1], 1)
        signal(ready.at[2], beside)

    @pl.when(side == 1)
    def _():
        pl.semaphore_wait(ready.at[2], 1)

    for send in ahead:
        send.start()

    def far_group(at, carry):
        lse_send(at).wait_recv()
        q_send(at).wait_recv()
        theirs = lse_peer[at]
        units = units_of(at)
        parts, totals, stats = partial_attentions(
            [q_far[branch, :, cols] for branch, cols, _ in units],
            [k_all[branch, :, cols] for branch, cols, _ in units],
            [v_all[branch, :, cols] for branch, cols, _ in units],
        )
        lse = jnp.zeros((TILE, HDIM), jnp.float32)
        terms = []
        for (branch, cols, spot), part, total, stat in zip(units, parts, totals, stats):
            lse = pack(stat, spot, lse)
            factor = (GUIDANCE, 1.0 - GUIDANCE)[branch]
            terms.append(part * (factor * share(stat, unpack(theirs, spot, rows)) / total))
        for extra in range(HEADS_AT_ONCE):
            pair = terms[extra * branches] + terms[extra * branches + 1]
            part_far[:, head_span(at, extra)] = pair.astype(jnp.bfloat16)
        lse_far[at] = lse
        stat_send(at).start()

        @pl.when(at < last)
        def _():
            back_send(span(at), at).start()

        return carry

    lax.fori_loop(0, groups, far_group, 0)
    for cols, piece in endings:
        back_send(cols, piece).start()

    for send in ahead:
        send.wait_recv()
    trade_row = jnp.broadcast_to(flags[...], (1, width)) == 1
    gain_next[...] = jnp.where(trade_row, gain_peer[...], gain_move[...])
    trade = jnp.broadcast_to(flags[...], (rows, HDIM)) == 1

    def finish_head(weight, cols, spot):
        value = (
            GUIDANCE * unpack(weight, spot, rows) * part_own[0, :, cols]
            + (1.0 - GUIDANCE) * unpack(weight, spot + 1, rows) * part_own[1, :, cols]
            + part_back[:, cols].astype(jnp.float32)
        ).astype(jnp.bfloat16)
        guided[:, cols] = value
        wide = value.astype(jnp.float32)
        squares[...] += wide * wide

    def meet_head(cols):
        theirs = guided_peer[:, cols].astype(jnp.float32)
        squares_peer[...] += theirs * theirs
        mine = guided[:, cols].astype(jnp.float32)
        lifted[:, cols] = gain_next[:, cols] * jnp.where(trade, theirs, mine)
        base[:, cols] = jnp.where(
            trade, now_peer[:, cols].astype(jnp.float32), now[:, cols].astype(jnp.float32)
        ).astype(jnp.bfloat16)

    def meet_group(at):
        cross_send(span(at), at).wait_recv()
        for extra in range(HEADS_AT_ONCE):
            meet_head(head_span(at, extra))

    def finish_group(at, carry):
        stat_send(at).wait_recv()
        back_send(span(at), at).wait_recv()
        weight = share(lse_own[at], lse_back[at])
        for extra in range(HEADS_AT_ONCE):
            finish_head(weight, head_span(at, extra), extra * branches)
        cross_send(span(at), at).start()

        @pl.when(at >= LAG)
        def _():
            meet_group(at - LAG)

        return carry

    lax.fori_loop(0, last, finish_group, 0)

    stat_send(last).wait_recv()
    weight = share(lse_own[last], lse_back[last])
    for extra, (cols, piece) in enumerate(endings):
        back_send(cols, piece).wait_recv()
        finish_head(weight, cols, extra * branches)
        cross_send(cols, piece).start()

    scale = lax.rsqrt(jnp.sum(squares[...], axis=-1, keepdims=True) / width + 1e-06)

    def denoise_group(at, carry):
        for extra in range(HEADS_AT_ONCE):
            cols = head_span(at, extra)
            unit = guided[:, cols].astype(jnp.float32) * scale
            denoised[:, cols] = (
                now[:, cols].astype(jnp.float32) - gain_now[:, cols] * unit
            ).astype(jnp.bfloat16)
        return carry

    lax.fori_loop(0, groups, denoise_group, 0)

    def meet_rest(at, carry):
        meet_group(at)
        return carry

    lax.fori_loop(max(last - LAG, 0), last, meet_rest, 0)
    for cols, piece in endings:
        cross_send(cols, piece).wait_recv()
        meet_head(cols)
    scale_peer = lax.rsqrt(jnp.sum(squares_peer[...], axis=-1, keepdims=True) / width + 1e-06)
    scale_out[...] = jnp.where(trade, scale_peer, scale)

    def drain(at, carry):
        for send in (q_send(at), lse_send(at), stat_send(at)) + kv_sends(at):
            send.wait_send()
        return carry

    def drain_pieces(at, carry):
        for send in (back_send(span(at), at), cross_send(span(at), at)):
            send.wait_send()
        return carry

    lax.fori_loop(0, groups, drain, 0)
    lax.fori_loop(0, last, drain_pieces, 0)
    for cols, piece in endings:
        back_send(cols, piece).wait_send()
        cross_send(cols, piece).wait_send()
    for send in ahead:
        send.wait_send()


def place_kernel(denoised_in, lifted, base, scale, denoised, next_latents, rows_out, sems):
    rows, width = base.shape
    group = HEADS_AT_ONCE * HDIM
    groups = width // group
    whole = pltpu.make_async_copy(denoised_in, denoised, sems.at[groups])
    whole.start()

    def span(at):
        return pl.ds(pl.multiple_of(at * group, group), group)

    def store(at):
        return pltpu.make_async_copy(rows_out.at[:, span(at)], next_latents.at[:, span(at)], sems.at[at])

    def move_group(at, carry):
        for extra in range(HEADS_AT_ONCE):
            cols = pl.ds(pl.multiple_of(at * group + extra * HDIM, HDIM), HDIM)
            rows_out[:, cols] = (
                base[:, cols].astype(jnp.float32) + lifted[:, cols] * scale[...]
            ).astype(jnp.bfloat16)
        store(at).start()
        return carry

    lax.fori_loop(0, groups, move_group, 0)

    def drain(at, carry):
        store(at).wait()
        return carry

    lax.fori_loop(0, groups, drain, 0)
    whole.wait()


def exchange_queries(queries, keys, values, latents, gain, steps_table, flags):
    branches, rows, width = queries.shape[2:]
    groups = width // (HEADS_AT_ONCE * HDIM)
    pieces = groups - 1 + HEADS_AT_ONCE
    low = functools.partial(pltpu.VMEM, dtype=jnp.bfloat16)
    high = functools.partial(pltpu.VMEM, dtype=jnp.float32)
    dma = pltpu.SemaphoreType.DMA
    hbm = pl.BlockSpec(memory_space=pltpu.HBM)
    vmem = pl.BlockSpec(memory_space=pltpu.VMEM)
    stats = high((groups, TILE, HDIM))
    results = pl.pallas_call(
        pair_kernel,
        out_shape=(low((rows, width)), high((rows, width)), low((rows, width)), high((rows, HDIM))),
        in_specs=[hbm] * 7,
        out_specs=(vmem,) * 4,
        scratch_shapes=[
            low((branches, rows, width)),
            low((branches, rows, width)),
            low((branches, 2 * rows, width)),
            low((branches, 2 * rows, width)),
            high((branches, rows, width)),
            low((rows, width)),
            low((rows, width)),
            low((rows, width)),
            low((rows, width)),
            low((rows, width)),
            low((rows, width)),
            stats,
            stats,
            stats,
            stats,
            high((rows, HDIM)),
            high((rows, HDIM)),
            low((1, width)),
            pltpu.VMEM((1, 1), jnp.int32),
            pltpu.VMEM((1, 1), jnp.int32),
            high((1, width)),
            high((1, width)),
            high((1, width)),
            high((1, width)),
            dma((7,)),
            dma((2, 2 * groups)),
            dma((2, groups)),
            dma((2, groups)),
            dma((2, pieces)),
            dma((2, groups)),
            dma((2, pieces)),
            dma((2, 2)),
            pltpu.SemaphoreType.REGULAR((3,)),
        ],
        compiler_params=pltpu.CompilerParams(collective_id=0, has_side_effects=True),
    )(
        queries[0, 0], keys[0, 0], values[0, 0], latents[0, 0], gain, steps_table,
        flags.reshape(1, 1),
    )
    whole = jax.ShapeDtypeStruct((rows, width), jnp.bfloat16)
    denoised, next_latents = pl.pallas_call(
        place_kernel,
        out_shape=(whole, whole),
        in_specs=[vmem] * 4,
        out_specs=(hbm, hbm),
        scratch_shapes=[low((rows, width)), dma((groups + 1,))],
    )(*(pltpu.with_memory_space_constraint(part, pltpu.VMEM) for part in results))
    return (denoised[None, None], next_latents[None, None])


def per_device(*blocks):
    branches, rows, width = blocks[0].shape[2:]
    paired = (
        lax.axis_size("seq") == 2 * 2
        and lax.axis_size("expert") == 2
        and branches == 2
        and rows % (2 * TILE) == 0
        and rows // TILE * HEADS_AT_ONCE * branches <= HDIM
        and HEADS_AT_ONCE * branches <= TILE
        and width % (HEADS_AT_ONCE * HDIM) == 0
    )
    return (exchange_queries if paired else exchange_heads)(*blocks)


def solution(mesh):
    placed = (
        P("expert", "batch", None, "seq", None),
        P("expert", "batch", None, "seq", None),
        P("expert", "batch", None, "seq", None),
        P("expert", "batch", "seq", None),
        P("expert", None),
        P("expert", "batch"),
        P("batch"),
    )
    return jax.shard_map(
        per_device,
        mesh=mesh,
        in_specs=placed,
        out_specs=(P("expert", "batch", "seq", None), P("expert", "batch", "seq", None)),
        check_vma=False,
    )
```

```python
import functools

import jax
import jax.numpy as jnp
from jax import lax
from jax.experimental import pallas as pl
from jax.experimental.pallas import tpu as pltpu
from jax.sharding import PartitionSpec as P

HDIM = 128
STEPS = 40


GUIDANCE = 3.5
flow_shift = 5.0


def from_partner(block, axis, bit):
    count = lax.axis_size(axis)
    route = []
    for low in range(count):
        high = low | 1 << bit
        if high != low and high < count:
            route += [(low, high), (high, low)]
    return lax.ppermute(block, axis, route)


def sigma_of(step):
    level = 1.0 - step.astype(jnp.float32) / STEPS
    return flow_shift * level / (1.0 + (flow_shift - 1.0) * level)


def combine(cond, uncond):
    base = uncond.astype(jnp.float32)
    return (base + GUIDANCE * (cond.astype(jnp.float32) - base)).astype(jnp.bfloat16)


def attend(stacked):
    query_heads, key_heads, value_heads = stacked
    items, length, width_dev = query_heads.shape
    heads_dev = width_dev // HDIM
    block = 512 if length % 512 == 0 else length
    key_rows = key_heads.reshape(items, length, heads_dev, HDIM)
    value_rows = value_heads.reshape(items, length, heads_dev, HDIM)
    query_blocks = query_heads.reshape(items, length // block, block, heads_dev, HDIM).transpose(
        1, 0, 2, 3, 4
    )

    def one_block(query_part):
        scores = jnp.einsum(
            "nqhd,nkhd->nhqk", query_part, key_rows, preferred_element_type=jnp.float32
        ) * HDIM ** (-0.5)
        weights = jax.nn.softmax(scores, axis=-1).astype(jnp.bfloat16)
        return jnp.einsum(
            "nhqk,nkhd->nqhd", weights, value_rows, preferred_element_type=jnp.float32
        ).astype(jnp.bfloat16)

    result = lax.map(one_block, query_blocks)
    return result.transpose(1, 0, 2, 3, 4).reshape(items, length, width_dev)


def exchange_heads(queries, keys, values, latents, gain, steps_table, flags):
    attended = attend(
        (
            lax.all_to_all(queries[0, 0], "seq", split_axis=2, concat_axis=1, tiled=True),
            lax.all_to_all(keys[0, 0], "seq", split_axis=2, concat_axis=1, tiled=True),
            lax.all_to_all(values[0, 0], "seq", split_axis=2, concat_axis=1, tiled=True),
        )
    )
    guided = lax.all_to_all(
        combine(attended[0], attended[1]), "seq", split_axis=0, concat_axis=1, tiled=True
    )
    guided_f32 = guided.astype(jnp.float32)
    scale = lax.rsqrt(jnp.mean(guided_f32 * guided_f32, axis=-1, keepdims=True) + 1e-06)
    velocity = guided_f32 * scale * gain[0].astype(jnp.float32)[None, :]
    step_now = steps_table[0, 0]
    sigma_now = sigma_of(step_now)
    sigma_next = sigma_of(step_now + 1)
    current = latents[0, 0].astype(jnp.float32)
    denoised = (current - sigma_now * velocity).astype(jnp.bfloat16)
    moved = (current + (sigma_next - sigma_now) * velocity).astype(jnp.bfloat16)
    partner = from_partner(moved, "expert", 0)
    next_latents = jnp.where(flags[0] == 1, partner, moved)
    return (denoised[None, None], next_latents[None, None])


MESH = pl.DeviceIdType.MESH
HEADS_AT_ONCE = 4
AHEAD = 5
FIRST = 2
PIECE = 2
LAG = 2
MEET = AHEAD + LAG
TILE = 8
LOG2E = 1.4426950408889634


def partial_attentions(queries, key_blocks, value_blocks):
    scores = [
        lax.dot_general(query, rows, (((1,), (1,)), ((), ())), preferred_element_type=jnp.float32)
        for query, rows in zip(queries, key_blocks)
    ]
    tops = [jnp.max(score, axis=-1, keepdims=True) for score in scores]
    powers = [
        jnp.exp2((score - top) * (HDIM ** (-0.5) * LOG2E)).astype(jnp.bfloat16)
        for score, top in zip(scores, tops)
    ]
    ones = jnp.ones_like(value_blocks[0])
    sums = [
        jnp.dot(
            power, jnp.concatenate([rows, ones], axis=1), preferred_element_type=jnp.float32
        )
        for power, rows in zip(powers, value_blocks)
    ]
    parts = [both[:, :HDIM] for both in sums]
    totals = [both[:, HDIM:] for both in sums]
    stats = [
        top * (HDIM ** (-0.5) * LOG2E) + jnp.log2(total[:, :1]) for top, total in zip(tops, totals)
    ]
    return parts, totals, stats


def share(mine, other):
    return 1.0 / (1.0 + jnp.exp2(other - mine))


def pack(stat, spot, packed):
    lane = lax.broadcasted_iota(jnp.int32, packed.shape, 1)
    for at in range(stat.shape[0] // TILE):
        here = stat[at * TILE : (at + 1) * TILE]
        packed = jnp.where(lane == at * TILE + spot, here, packed)
    return packed


def unpack(packed, spot, rows):
    return jnp.concatenate(
        [packed[:, at * TILE + spot : at * TILE + spot + 1] for at in range(rows // TILE)], axis=0
    )


def pair_kernel(
    queries, keys, values, latents, gain_in, steps_in, flags_in,
    denoised, lifted, base, scale_out,
    q_own, q_far, k_all, v_all, part_own, part_far, part_back, guided, guided_peer,
    now, now_peer, lse_own, lse_peer, lse_far, lse_back, squares, squares_peer,
    gain, steps, flags, gain_now, gain_move, gain_peer, gain_next,
    load_sems, kv_sems, q_sems, lse_sems, back_sems, stat_sems, cross_sems, ahead_sems, ready,
):
    seq = lax.axis_index("seq")
    size = lax.axis_size("seq")
    side = lax.rem(seq, 2)
    beside = {"seq": seq + 1 - 2 * side}
    across = {"seq": lax.rem(seq + size // 2, size)}
    other = {"expert": 1 - lax.axis_index("expert")}
    branches, rows, width = queries.shape
    group = HEADS_AT_ONCE * HDIM
    groups = width // group
    last = groups - 1

    def signal(sem, peer):
        pl.semaphore_signal(sem, inc=1, device_id=peer, device_id_type=MESH)

    barrier = pltpu.get_barrier_semaphore()
    signal(barrier, across)

    @pl.when(side == 0)
    def _():
        signal(barrier, other)
        signal(barrier, beside)

    own_keys = pl.ds(0, rows)
    peer_keys = pl.ds(rows, rows)
    loads = [
        pltpu.make_async_copy(steps_in, steps, load_sems.at[0]),
        pltpu.make_async_copy(flags_in, flags, load_sems.at[1]),
        pltpu.make_async_copy(gain_in, gain, load_sems.at[2]),
        pltpu.make_async_copy(queries, q_own, load_sems.at[3]),
        pltpu.make_async_copy(keys, k_all.at[:, own_keys], load_sems.at[4]),
        pltpu.make_async_copy(values, v_all.at[:, own_keys], load_sems.at[5]),
        pltpu.make_async_copy(latents, now, load_sems.at[6]),
    ]
    for load in loads:
        load.start()
    pl.semaphore_wait(barrier, 2)

    def remote(source, target, sems, index, peer):
        return pltpu.make_async_remote_copy(
            src_ref=source, dst_ref=target, send_sem=sems.at[0, index],
            recv_sem=sems.at[1, index], device_id=peer, device_id_type=MESH,
        )

    def span(at):
        return pl.ds(pl.multiple_of(at * group, group), group)

    def head_span(at, extra):
        return pl.ds(pl.multiple_of(at * group + extra * HDIM, HDIM), HDIM)

    def q_send(at):
        cols = span(at)
        return remote(queries.at[:, :, cols], q_far.at[:, :, cols], q_sems, at, across)

    def kv_sends(at):
        cols = span(at)
        return (
            remote(keys.at[:, :, cols], k_all.at[:, peer_keys, cols], kv_sems, 2 * at, beside),
            remote(values.at[:, :, cols], v_all.at[:, peer_keys, cols], kv_sems, 2 * at + 1, beside),
        )

    def lse_send(at):
        return remote(lse_own.at[at], lse_peer.at[at], lse_sems, at, across)

    def stat_send(at):
        return remote(lse_far.at[at], lse_back.at[at], stat_sems, at, across)

    def back_send(first, many, piece):
        heads = pl.ds(first, many)
        return remote(part_far.at[heads], part_back.at[heads], back_sems, piece, across)

    def cross_send(first, many, piece):
        heads = pl.ds(first, many)
        return remote(guided.at[heads], guided_peer.at[heads], cross_sems, piece, other)

    cuts = HEADS_AT_ONCE // PIECE

    def pieces_of(at):
        return [
            (at * HEADS_AT_ONCE + cut * PIECE, PIECE, at * cuts + cut) for cut in range(cuts)
        ]

    endings = [
        (last * HEADS_AT_ONCE + extra, 1, last * cuts + extra) for extra in range(HEADS_AT_ONCE)
    ]

    for at in range(FIRST):
        q_send(at).start()

    def start_kv():
        def step(at, carry):
            for send in kv_sends(at):
                send.start()
            return carry

        lax.fori_loop(0, groups, step, 0)

    ahead = [
        remote(latents, now_peer, ahead_sems, 0, other),
        remote(gain_move, gain_peer, ahead_sems, 1, other),
    ]

    @pl.when(side == 0)
    def _():
        pl.semaphore_wait(ready.at[0], 1)
        signal(ready.at[1], other)

    @pl.when(side == 1)
    def _():
        signal(ready.at[0], beside)

    start_kv()

    for load in loads[:3]:
        load.wait()
    step = jnp.broadcast_to(steps[...], (1, HDIM))
    sigma_now = sigma_of(step)[:, :1]
    sigma_next = sigma_of(step + 1)[:, :1]
    row = gain[...].astype(jnp.float32)
    gain_now[...] = sigma_now * row
    gain_move[...] = (sigma_next - sigma_now) * row
    squares[...] = jnp.zeros_like(squares)
    squares_peer[...] = jnp.zeros_like(squares_peer)
    for load in loads[3:]:
        load.wait()

    def units_of(at):
        return [
            (branch, head_span(at, extra), extra * branches + branch)
            for extra in range(HEADS_AT_ONCE)
            for branch in range(branches)
        ]

    def own_group(at, carry):
        for send in kv_sends(at):
            send.wait_recv()
        units = units_of(at)
        parts, totals, stats = partial_attentions(
            [q_own[branch, :, cols] for branch, cols, _ in units],
            [k_all[branch, :, cols] for branch, cols, _ in units],
            [v_all[branch, :, cols] for branch, cols, _ in units],
        )
        lse = jnp.zeros((TILE, HDIM), jnp.float32)
        for (branch, cols, spot), part, total, stat in zip(units, parts, totals, stats):
            part_own[branch, :, cols] = part / total
            lse = pack(stat, spot, lse)
        lse_own[at] = lse
        lse_send(at).start()

        @pl.when(at < AHEAD - FIRST)
        def _():
            q_send(at + FIRST).start()

        return carry

    lax.fori_loop(0, groups, own_group, 0)

    @pl.when(side == 0)
    def _():
        pl.semaphore_wait(ready.at[1], 1)
        signal(ready.at[2], beside)

    @pl.when(side == 1)
    def _():
        pl.semaphore_wait(ready.at[2], 1)

    for send in ahead:
        send.start()

    def far_group(at):
        lse_send(at).wait_recv()

        q_send(at).wait_recv()
        theirs = lse_peer[at]
        units = units_of(at)
        parts, totals, stats = partial_attentions(
            [q_far[branch, :, cols] for branch, cols, _ in units],
            [k_all[branch, :, cols] for branch, cols, _ in units],
            [v_all[branch, :, cols] for branch, cols, _ in units],
        )
        lse = jnp.zeros((TILE, HDIM), jnp.float32)
        terms = []
        for (branch, cols, spot), part, total, stat in zip(units, parts, totals, stats):
            lse = pack(stat, spot, lse)
            factor = (GUIDANCE, 1.0 - GUIDANCE)[branch]
            terms.append(part * (factor * share(stat, unpack(theirs, spot, rows)) / total))
        for extra in range(HEADS_AT_ONCE):
            pair = terms[extra * branches] + terms[extra * branches + 1]
            part_far[at * HEADS_AT_ONCE + extra] = pair.astype(jnp.bfloat16)
        lse_far[at] = lse
        stat_send(at).start()

        @pl.when(at < last)
        def _():
            for piece in pieces_of(at):
                back_send(*piece).start()

        @pl.when(at + AHEAD < groups)
        def _():
            q_send(at + AHEAD).start()

    trade = jnp.broadcast_to(flags[...], (rows, HDIM)) == 1

    def own_term(weight, at, extra):
        cols = head_span(at, extra)
        spot = extra * branches
        return (
            GUIDANCE * unpack(weight, spot, rows) * part_own[0, :, cols]
            + (1.0 - GUIDANCE) * unpack(weight, spot + 1, rows) * part_own[1, :, cols]
        )

    def finish_head(term, head):
        value = (term + part_back[head].astype(jnp.float32)).astype(jnp.bfloat16)
        guided[head] = value
        wide = value.astype(jnp.float32)
        squares[...] += wide * wide

    def meet_head(at, extra):
        cols = head_span(at, extra)
        head = at * HEADS_AT_ONCE + extra
        theirs = guided_peer[head].astype(jnp.float32)
        squares_peer[...] += theirs * theirs
        mine = guided[head].astype(jnp.float32)
        lifted[:, cols] = gain_next[:, cols] * jnp.where(trade, theirs, mine)
        base[:, cols] = jnp.where(
            trade, now_peer[:, cols].astype(jnp.float32), now[:, cols].astype(jnp.float32)
        ).astype(jnp.bfloat16)

    def meet_group(at):
        for piece in pieces_of(at):
            cross_send(*piece).wait_recv()
        for extra in range(HEADS_AT_ONCE):
            meet_head(at, extra)

    def finish_group(at):
        stat_send(at).wait_recv()
        weight = share(lse_own[at], lse_back[at])
        terms = [own_term(weight, at, extra) for extra in range(HEADS_AT_ONCE)]
        for cut, piece in enumerate(pieces_of(at)):
            back_send(*piece).wait_recv()
            for extra in range(cut * PIECE, (cut + 1) * PIECE):
                finish_head(terms[extra], at * HEADS_AT_ONCE + extra)
            cross_send(*piece).start()

    def step_group(at, carry):
        @pl.when(at >= AHEAD)
        def _():
            finish_group(at - AHEAD)

        far_group(at)

        @pl.when(at == MEET)
        def _():
            for send in ahead:
                send.wait_recv()
            trade_row = jnp.broadcast_to(flags[...], (1, width)) == 1
            gain_next[...] = jnp.where(trade_row, gain_peer[...], gain_move[...])

        @pl.when(at >= MEET)
        def _():
            meet_group(at - MEET)

        return carry

    lax.fori_loop(0, groups, step_group, 0)
    for piece in endings:
        back_send(*piece).start()

    def late_group(at, carry):
        finish_group(at)
        meet_group(at - LAG)
        return carry

    lax.fori_loop(groups - AHEAD, last, late_group, 0)

    stat_send(last).wait_recv()
    weight = share(lse_own[last], lse_back[last])
    for extra in range(HEADS_AT_ONCE):
        part_own[0, :, head_span(last, extra)] = own_term(weight, last, extra)
    for extra, piece in enumerate(endings):
        back_send(*piece).wait_recv()
        finish_head(part_own[0, :, head_span(last, extra)], piece[0])
        cross_send(*piece).start()

    scale = lax.rsqrt(jnp.sum(squares[...], axis=-1, keepdims=True) / width + 1e-06)

    def denoise_group(at, carry):
        for extra in range(HEADS_AT_ONCE):
            cols = head_span(at, extra)
            unit = guided[at * HEADS_AT_ONCE + extra].astype(jnp.float32) * scale
            denoised[:, cols] = (
                now[:, cols].astype(jnp.float32) - gain_now[:, cols] * unit
            ).astype(jnp.bfloat16)
        return carry

    lax.fori_loop(0, groups, denoise_group, 0)

    def drain(at, carry):
        for send in (lse_send(at), stat_send(at)) + kv_sends(at):
            send.wait_send()
        return carry

    def drain_groups(at, carry):
        for piece in pieces_of(at):
            back_send(*piece).wait_send()
            cross_send(*piece).wait_send()
        return carry

    def drain_queries(at, carry):
        q_send(at).wait_send()
        return carry

    lax.fori_loop(0, groups, drain, 0)
    lax.fori_loop(0, last, drain_groups, 0)
    lax.fori_loop(0, groups, drain_queries, 0)
    for send in ahead:
        send.wait_send()
    for piece in endings:
        back_send(*piece).wait_send()
    for at in range(last - LAG, last):
        meet_group(at)
    for extra, piece in enumerate(endings):
        cross_send(*piece).wait_recv()
        meet_head(last, extra)
    scale_peer = lax.rsqrt(jnp.sum(squares_peer[...], axis=-1, keepdims=True) / width + 1e-06)
    scale_out[...] = jnp.where(trade, scale_peer, scale)
    for piece in endings:
        cross_send(*piece).wait_send()


def place_kernel(denoised_in, lifted, base, scale, denoised, next_latents, rows_out, sems):
    rows, width = base.shape
    group = HEADS_AT_ONCE * HDIM
    groups = width // group
    whole = pltpu.make_async_copy(denoised_in, denoised, sems.at[groups])
    whole.start()

    stores = [whole]
    for at in range(groups):
        for extra in range(HEADS_AT_ONCE):
            cols = pl.ds(at * group + extra * HDIM, HDIM)
            rows_out[:, cols] = (
                base[:, cols].astype(jnp.float32) + lifted[:, cols] * scale[...]
            ).astype(jnp.bfloat16)
        here = pl.ds(at * group, group)
        stores.append(
            pltpu.make_async_copy(rows_out.at[:, here], next_latents.at[:, here], sems.at[at])
        )
        stores[-1].start()
    for store in stores:
        store.wait()


def exchange_queries(queries, keys, values, latents, gain, steps_table, flags):
    branches, rows, width = queries.shape[2:]
    groups = width // (HEADS_AT_ONCE * HDIM)
    pieces = (groups - 1) * (HEADS_AT_ONCE // PIECE) + HEADS_AT_ONCE
    low = functools.partial(pltpu.VMEM, dtype=jnp.bfloat16)
    high = functools.partial(pltpu.VMEM, dtype=jnp.float32)
    dma = pltpu.SemaphoreType.DMA
    hbm = pl.BlockSpec(memory_space=pltpu.HBM)
    vmem = pl.BlockSpec(memory_space=pltpu.VMEM)
    stats = high((groups, TILE, HDIM))
    by_head = low((width // HDIM, rows, HDIM))
    results = pl.pallas_call(
        pair_kernel,
        out_shape=(low((rows, width)), high((rows, width)), low((rows, width)), high((rows, HDIM))),
        in_specs=[hbm] * 7,
        out_specs=(vmem,) * 4,
        scratch_shapes=[
            low((branches, rows, width)),
            low((branches, rows, width)),
            low((branches, 2 * rows, width)),
            low((branches, 2 * rows, width)),
            high((branches, rows, width)),
            by_head,
            by_head,
            by_head,
            by_head,
            low((rows, width)),
            low((rows, width)),
            stats,
            stats,
            stats,
            stats,
            high((rows, HDIM)),
            high((rows, HDIM)),
            low((1, width)),
            pltpu.VMEM((1, 1), jnp.int32),
            pltpu.VMEM((1, 1), jnp.int32),
            high((1, width)),
            high((1, width)),
            high((1, width)),
            high((1, width)),
            dma((7,)),
            dma((2, 2 * groups)),
            dma((2, groups)),
            dma((2, groups)),
            dma((2, pieces)),
            dma((2, groups)),
            dma((2, pieces)),
            dma((2, 2)),
            pltpu.SemaphoreType.REGULAR((3,)),
        ],
        compiler_params=pltpu.CompilerParams(collective_id=0, has_side_effects=True),
    )(
        queries[0, 0], keys[0, 0], values[0, 0], latents[0, 0], gain, steps_table,
        flags.reshape(1, 1),
    )
    whole = jax.ShapeDtypeStruct((rows, width), jnp.bfloat16)
    denoised, next_latents = pl.pallas_call(
        place_kernel,
        out_shape=(whole, whole),
        in_specs=[vmem] * 4,
        out_specs=(hbm, hbm),
        scratch_shapes=[low((rows, width)), dma((groups + 1,))],
    )(*(pltpu.with_memory_space_constraint(part, pltpu.VMEM) for part in results))
    return (denoised[None, None], next_latents[None, None])


def per_device(*blocks):
    branches, rows, width = blocks[0].shape[2:]
    paired = (
        lax.axis_size("seq") == 2 * 2
        and lax.axis_size("expert") == 2
        and branches == 2
        and rows % (2 * TILE) == 0
        and rows // TILE * HEADS_AT_ONCE * branches <= HDIM
        and HEADS_AT_ONCE * branches <= TILE
        and width % (HEADS_AT_ONCE * HDIM) == 0
        and width // (HEADS_AT_ONCE * HDIM) > MEET
    )
    return (exchange_queries if paired else exchange_heads)(*blocks)


def solution(mesh):
    placed = (
        P("expert", "batch", None, "seq", None),
        P("expert", "batch", None, "seq", None),
        P("expert", "batch", None, "seq", None),
        P("expert", "batch", "seq", None),
        P("expert", None),
        P("expert", "batch"),
        P("batch"),
    )
    return jax.shard_map(
        per_device,
        mesh=mesh,
        in_specs=placed,
        out_specs=(P("expert", "batch", "seq", None), P("expert", "batch", "seq", None)),
        check_vma=False,
    )
```

```python
import functools

import jax
import jax.numpy as jnp
from jax import lax
from jax.experimental import pallas as pl
from jax.experimental.pallas import tpu as pltpu
from jax.sharding import PartitionSpec as P

HDIM = 128
STEPS = 40


GUIDANCE = 3.5
flow_shift = 5.0


def from_partner(block, axis, bit):
    count = lax.axis_size(axis)
    route = []
    for low in range(count):
        high = low | 1 << bit
        if high != low and high < count:
            route += [(low, high), (high, low)]
    return lax.ppermute(block, axis, route)


def sigma_of(step):
    level = 1.0 - step.astype(jnp.float32) / STEPS
    return flow_shift * level / (1.0 + (flow_shift - 1.0) * level)


def combine(cond, uncond):
    base = uncond.astype(jnp.float32)
    return (base + GUIDANCE * (cond.astype(jnp.float32) - base)).astype(jnp.bfloat16)


def attend(stacked):
    query_heads, key_heads, value_heads = stacked
    items, length, width_dev = query_heads.shape
    heads_dev = width_dev // HDIM
    block = 512 if length % 512 == 0 else length
    key_rows = key_heads.reshape(items, length, heads_dev, HDIM)
    value_rows = value_heads.reshape(items, length, heads_dev, HDIM)
    query_blocks = query_heads.reshape(items, length // block, block, heads_dev, HDIM).transpose(
        1, 0, 2, 3, 4
    )

    def one_block(query_part):
        scores = jnp.einsum(
            "nqhd,nkhd->nhqk", query_part, key_rows, preferred_element_type=jnp.float32
        ) * HDIM ** (-0.5)
        weights = jax.nn.softmax(scores, axis=-1).astype(jnp.bfloat16)
        return jnp.einsum(
            "nhqk,nkhd->nqhd", weights, value_rows, preferred_element_type=jnp.float32
        ).astype(jnp.bfloat16)

    result = lax.map(one_block, query_blocks)
    return result.transpose(1, 0, 2, 3, 4).reshape(items, length, width_dev)


def exchange_heads(queries, keys, values, latents, gain, steps_table, flags):
    attended = attend(
        (
            lax.all_to_all(queries[0, 0], "seq", split_axis=2, concat_axis=1, tiled=True),
            lax.all_to_all(keys[0, 0], "seq", split_axis=2, concat_axis=1, tiled=True),
            lax.all_to_all(values[0, 0], "seq", split_axis=2, concat_axis=1, tiled=True),
        )
    )
    guided = lax.all_to_all(
        combine(attended[0], attended[1]), "seq", split_axis=0, concat_axis=1, tiled=True
    )
    guided_f32 = guided.astype(jnp.float32)
    scale = lax.rsqrt(jnp.mean(guided_f32 * guided_f32, axis=-1, keepdims=True) + 1e-06)
    velocity = guided_f32 * scale * gain[0].astype(jnp.float32)[None, :]
    step_now = steps_table[0, 0]
    sigma_now = sigma_of(step_now)
    sigma_next = sigma_of(step_now + 1)
    current = latents[0, 0].astype(jnp.float32)
    denoised = (current - sigma_now * velocity).astype(jnp.bfloat16)
    moved = (current + (sigma_next - sigma_now) * velocity).astype(jnp.bfloat16)
    partner = from_partner(moved, "expert", 0)
    next_latents = jnp.where(flags[0] == 1, partner, moved)
    return (denoised[None, None], next_latents[None, None])


MESH = pl.DeviceIdType.MESH
HEADS_AT_ONCE = 4
AHEAD = 4
FIRST = 2
PIECE = 4
LAG = 2
MEET = AHEAD + LAG
TILE = 8
LOG2E = 1.4426950408889634


def partial_attentions(queries, key_blocks, value_blocks):
    scores = [
        lax.dot_general(query, rows, (((1,), (1,)), ((), ())), preferred_element_type=jnp.float32)
        for query, rows in zip(queries, key_blocks)
    ]
    tops = [jnp.max(score, axis=-1, keepdims=True) for score in scores]
    powers = [
        jnp.exp2((score - top) * (HDIM ** (-0.5) * LOG2E)).astype(jnp.bfloat16)
        for score, top in zip(scores, tops)
    ]
    ones = jnp.ones_like(value_blocks[0])
    sums = [
        jnp.dot(
            power, jnp.concatenate([rows, ones], axis=1), preferred_element_type=jnp.float32
        )
        for power, rows in zip(powers, value_blocks)
    ]
    parts = [both[:, :HDIM] for both in sums]
    totals = [both[:, HDIM:] for both in sums]
    stats = [
        top * (HDIM ** (-0.5) * LOG2E) + jnp.log2(total[:, :1]) for top, total in zip(tops, totals)
    ]
    return parts, totals, stats


def share(mine, other):
    return 1.0 / (1.0 + jnp.exp2(other - mine))


def pack(stat, spot, packed):
    lane = lax.broadcasted_iota(jnp.int32, packed.shape, 1)
    for at in range(stat.shape[0] // TILE):
        here = stat[at * TILE : (at + 1) * TILE]
        packed = jnp.where(lane == at * TILE + spot, here, packed)
    return packed


def unpack(packed, spot, rows):
    return jnp.concatenate(
        [packed[:, at * TILE + spot : at * TILE + spot + 1] for at in range(rows // TILE)], axis=0
    )


def pair_kernel(
    queries, keys, values, latents, gain_in, steps_in, flags_in,
    denoised, lifted, base, scale_out,
    q_own, q_far, k_all, v_all, part_own, part_far, part_back, guided, guided_peer,
    now, now_peer, lse_own, lse_peer, keep_far, keep_back, squares, squares_peer,
    gain, steps, flags, gain_now, gain_move, gain_peer, gain_next,
    load_sems, kv_sems, q_sems, lse_sems, back_sems, stat_sems, cross_sems, ahead_sems, ready,
):
    seq = lax.axis_index("seq")
    size = lax.axis_size("seq")
    side = lax.rem(seq, 2)
    beside = {"seq": seq + 1 - 2 * side}
    across = {"seq": lax.rem(seq + size // 2, size)}
    other = {"expert": 1 - lax.axis_index("expert")}
    branches, rows, width = queries.shape
    group = HEADS_AT_ONCE * HDIM
    groups = width // group
    last = groups - 1

    def signal(sem, peer):
        pl.semaphore_signal(sem, inc=1, device_id=peer, device_id_type=MESH)

    barrier = pltpu.get_barrier_semaphore()
    signal(barrier, across)

    @pl.when(side == 0)
    def _():
        signal(barrier, other)
        signal(barrier, beside)

    own_keys = pl.ds(0, rows)
    peer_keys = pl.ds(rows, rows)
    loads = [
        pltpu.make_async_copy(steps_in, steps, load_sems.at[0]),
        pltpu.make_async_copy(flags_in, flags, load_sems.at[1]),
        pltpu.make_async_copy(gain_in, gain, load_sems.at[2]),
        pltpu.make_async_copy(queries, q_own, load_sems.at[3]),
        pltpu.make_async_copy(keys, k_all.at[:, own_keys], load_sems.at[4]),
        pltpu.make_async_copy(values, v_all.at[:, own_keys], load_sems.at[5]),
        pltpu.make_async_copy(latents, now, load_sems.at[6]),
    ]
    for load in loads:
        load.start()
    pl.semaphore_wait(barrier, 2)

    def remote(source, target, sems, index, peer):
        return pltpu.make_async_remote_copy(
            src_ref=source, dst_ref=target, send_sem=sems.at[0, index],
            recv_sem=sems.at[1, index], device_id=peer, device_id_type=MESH,
        )

    def span(at):
        return pl.ds(pl.multiple_of(at * group, group), group)

    def head_span(at, extra):
        return pl.ds(pl.multiple_of(at * group + extra * HDIM, HDIM), HDIM)

    def q_send(at):
        cols = span(at)
        return remote(queries.at[:, :, cols], q_far.at[:, :, cols], q_sems, at, across)

    def kv_sends(at):
        cols = span(at)
        return (
            remote(keys.at[:, :, cols], k_all.at[:, peer_keys, cols], kv_sems, 2 * at, beside),
            remote(values.at[:, :, cols], v_all.at[:, peer_keys, cols], kv_sems, 2 * at + 1, beside),
        )

    def lse_send(at):
        return remote(lse_own.at[at], lse_peer.at[at], lse_sems, at, across)

    def stat_send(at):
        return remote(keep_far.at[at], keep_back.at[at], stat_sems, at, across)

    def back_send(first, many, piece):
        heads = pl.ds(first, many)
        return remote(part_far.at[heads], part_back.at[heads], back_sems, piece, across)

    def cross_send(first, many, piece):
        heads = pl.ds(first, many)
        return remote(guided.at[heads], guided_peer.at[heads], cross_sems, piece, other)

    cuts = HEADS_AT_ONCE // PIECE

    def pieces_of(at):
        return [
            (at * HEADS_AT_ONCE + cut * PIECE, PIECE, at * cuts + cut) for cut in range(cuts)
        ]

    late = groups - AHEAD

    def singles_of(at):
        return [
            (at * HEADS_AT_ONCE + extra, 1, late * cuts + (at - late) * HEADS_AT_ONCE + extra)
            for extra in range(HEADS_AT_ONCE)
        ]

    for at in range(FIRST):
        q_send(at).start()

    def start_kv():
        def step(at, carry):
            for send in kv_sends(at):
                send.start()
            return carry

        lax.fori_loop(0, groups, step, 0)

    ahead = [
        remote(latents, now_peer, ahead_sems, 0, other),
        remote(gain_move, gain_peer, ahead_sems, 1, other),
    ]

    @pl.when(side == 0)
    def _():
        pl.semaphore_wait(ready.at[0], 1)
        signal(ready.at[1], other)

    @pl.when(side == 1)
    def _():
        signal(ready.at[0], beside)

    start_kv()

    for load in loads[:3]:
        load.wait()
    step = jnp.broadcast_to(steps[...], (1, HDIM))
    sigma_now = sigma_of(step)[:, :1]
    sigma_next = sigma_of(step + 1)[:, :1]
    row = gain[...].astype(jnp.float32)
    gain_now[...] = sigma_now * row
    gain_move[...] = (sigma_next - sigma_now) * row
    squares[...] = jnp.zeros_like(squares)
    squares_peer[...] = jnp.zeros_like(squares_peer)
    for load in loads[3:]:
        load.wait()

    def units_of(at):
        return [
            (branch, head_span(at, extra), extra * branches + branch)
            for extra in range(HEADS_AT_ONCE)
            for branch in range(branches)
        ]

    def own_group(at, carry):
        for send in kv_sends(at):
            send.wait_recv()
        units = units_of(at)
        parts, totals, stats = partial_attentions(
            [q_own[branch, :, cols] for branch, cols, _ in units],
            [k_all[branch, :, cols] for branch, cols, _ in units],
            [v_all[branch, :, cols] for branch, cols, _ in units],
        )
        lse = jnp.zeros((TILE, HDIM), jnp.float32)
        for (branch, cols, spot), part, total, stat in zip(units, parts, totals, stats):
            part_own[branch, :, cols] = part / total
            lse = pack(stat, spot, lse)
        lse_own[at] = lse
        lse_send(at).start()

        @pl.when(at < AHEAD - FIRST)
        def _():
            q_send(at + FIRST).start()

        return carry

    lax.fori_loop(0, groups, own_group, 0)

    @pl.when(side == 0)
    def _():
        pl.semaphore_wait(ready.at[1], 1)
        signal(ready.at[2], beside)

    @pl.when(side == 1)
    def _():
        pl.semaphore_wait(ready.at[2], 1)

    for send in ahead:
        send.start()

    def far_group(at):
        lse_send(at).wait_recv()

        q_send(at).wait_recv()
        theirs = lse_peer[at]
        units = units_of(at)
        parts, totals, stats = partial_attentions(
            [q_far[branch, :, cols] for branch, cols, _ in units],
            [k_all[branch, :, cols] for branch, cols, _ in units],
            [v_all[branch, :, cols] for branch, cols, _ in units],
        )
        lse = jnp.zeros((TILE, HDIM), jnp.float32)
        terms = []
        for (branch, cols, spot), part, total, stat in zip(units, parts, totals, stats):
            lse = pack(stat, spot, lse)
            factor = (GUIDANCE, 1.0 - GUIDANCE)[branch]
            terms.append(part * (factor * share(stat, unpack(theirs, spot, rows)) / total))
        for extra in range(HEADS_AT_ONCE):
            pair = terms[extra * branches] + terms[extra * branches + 1]
            part_far[at * HEADS_AT_ONCE + extra] = pair.astype(jnp.bfloat16)
        keep_far[at] = share(theirs, lse).astype(jnp.bfloat16)
        stat_send(at).start()

        @pl.when(at < late)
        def _():
            for piece in pieces_of(at):
                back_send(*piece).start()

        @pl.when(at >= late)
        def _():
            for piece in singles_of(at):
                back_send(*piece).start()

        @pl.when(at + AHEAD < groups)
        def _():
            q_send(at + AHEAD).start()

    trade = jnp.broadcast_to(flags[...], (rows, HDIM)) == 1

    def own_term(weight, at, extra):
        cols = head_span(at, extra)
        spot = extra * branches
        return (
            GUIDANCE * unpack(weight, spot, rows) * part_own[0, :, cols]
            + (1.0 - GUIDANCE) * unpack(weight, spot + 1, rows) * part_own[1, :, cols]
        )

    def finish_head(term, head):
        value = (term + part_back[head].astype(jnp.float32)).astype(jnp.bfloat16)
        guided[head] = value
        wide = value.astype(jnp.float32)
        squares[...] += wide * wide

    def meet_head(at, extra):
        cols = head_span(at, extra)
        head = at * HEADS_AT_ONCE + extra
        theirs = guided_peer[head].astype(jnp.float32)
        squares_peer[...] += theirs * theirs
        mine = guided[head].astype(jnp.float32)
        lifted[:, cols] = gain_next[:, cols] * jnp.where(trade, theirs, mine)
        base[:, cols] = jnp.where(
            trade, now_peer[:, cols].astype(jnp.float32), now[:, cols].astype(jnp.float32)
        ).astype(jnp.bfloat16)

    def meet_group(at, pieces):
        for piece in pieces:
            cross_send(*piece).wait_recv()
        for extra in range(HEADS_AT_ONCE):
            meet_head(at, extra)

    def finish_group(at, pieces):
        stat_send(at).wait_recv()
        weight = keep_back[at].astype(jnp.float32)
        terms = [own_term(weight, at, extra) for extra in range(HEADS_AT_ONCE)]
        for piece in pieces:
            back_send(*piece).wait_recv()
            many = piece[1]
            for extra in range(many):
                finish_head(terms.pop(0), piece[0] + extra)
            cross_send(*piece).start()

    def step_group(at, carry):
        @pl.when(at >= AHEAD)
        def _():
            finish_group(at - AHEAD, pieces_of(at - AHEAD))

        far_group(at)

        @pl.when(at == MEET)
        def _():
            for send in ahead:
                send.wait_recv()
            trade_row = jnp.broadcast_to(flags[...], (1, width)) == 1
            gain_next[...] = jnp.where(trade_row, gain_peer[...], gain_move[...])

        @pl.when(at >= MEET)
        def _():
            meet_group(at - MEET, pieces_of(at - MEET))

        return carry

    lax.fori_loop(0, groups, step_group, 0)
    def late_group(at, carry):
        finish_group(at, singles_of(at))

        @pl.when(at - LAG < late)
        def _():
            meet_group(at - LAG, pieces_of(at - LAG))

        @pl.when(at - LAG >= late)
        def _():
            meet_group(at - LAG, singles_of(at - LAG))

        return carry

    lax.fori_loop(late, last, late_group, 0)
    finish_group(last, singles_of(last))

    scale = lax.rsqrt(jnp.sum(squares[...], axis=-1, keepdims=True) / width + 1e-06)

    def denoise_group(at, carry):
        for extra in range(HEADS_AT_ONCE):
            cols = head_span(at, extra)
            unit = guided[at * HEADS_AT_ONCE + extra].astype(jnp.float32) * scale
            denoised[:, cols] = (
                now[:, cols].astype(jnp.float32) - gain_now[:, cols] * unit
            ).astype(jnp.bfloat16)
        return carry

    lax.fori_loop(0, groups, denoise_group, 0)

    def drain(at, carry):
        for send in (lse_send(at), stat_send(at)) + kv_sends(at):
            send.wait_send()
        return carry

    def drain_groups(at, carry):
        for piece in pieces_of(at):
            back_send(*piece).wait_send()
            cross_send(*piece).wait_send()
        return carry

    def drain_late(at, carry):
        for piece in singles_of(at):
            back_send(*piece).wait_send()
            cross_send(*piece).wait_send()
        return carry

    def drain_queries(at, carry):
        q_send(at).wait_send()
        return carry

    lax.fori_loop(0, groups, drain, 0)
    lax.fori_loop(0, late, drain_groups, 0)
    lax.fori_loop(late, last, drain_late, 0)
    lax.fori_loop(0, groups, drain_queries, 0)
    for send in ahead:
        send.wait_send()
    for piece in singles_of(last):
        back_send(*piece).wait_send()
    for at in range(last - LAG, last):
        meet_group(at, singles_of(at) if at >= late else pieces_of(at))
    for extra, piece in enumerate(singles_of(last)):
        cross_send(*piece).wait_recv()
        meet_head(last, extra)
    scale_peer = lax.rsqrt(jnp.sum(squares_peer[...], axis=-1, keepdims=True) / width + 1e-06)
    scale_out[...] = jnp.where(trade, scale_peer, scale)
    for piece in singles_of(last):
        cross_send(*piece).wait_send()


def place_kernel(denoised_in, lifted, base, scale, denoised, next_latents, rows_out, sems):
    rows, width = base.shape
    group = HEADS_AT_ONCE * HDIM
    groups = width // group
    whole = pltpu.make_async_copy(denoised_in, denoised, sems.at[groups])
    whole.start()

    stores = [whole]
    for at in range(groups):
        for extra in range(HEADS_AT_ONCE):
            cols = pl.ds(at * group + extra * HDIM, HDIM)
            rows_out[:, cols] = (
                base[:, cols].astype(jnp.float32) + lifted[:, cols] * scale[...]
            ).astype(jnp.bfloat16)
        here = pl.ds(at * group, group)
        stores.append(
            pltpu.make_async_copy(rows_out.at[:, here], next_latents.at[:, here], sems.at[at])
        )
        stores[-1].start()
    for store in stores:
        store.wait()


def exchange_queries(queries, keys, values, latents, gain, steps_table, flags):
    branches, rows, width = queries.shape[2:]
    groups = width // (HEADS_AT_ONCE * HDIM)
    pieces = (groups - AHEAD) * (HEADS_AT_ONCE // PIECE) + AHEAD * HEADS_AT_ONCE
    low = functools.partial(pltpu.VMEM, dtype=jnp.bfloat16)
    high = functools.partial(pltpu.VMEM, dtype=jnp.float32)
    dma = pltpu.SemaphoreType.DMA
    hbm = pl.BlockSpec(memory_space=pltpu.HBM)
    vmem = pl.BlockSpec(memory_space=pltpu.VMEM)
    stats = high((groups, TILE, HDIM))
    by_head = low((width // HDIM, rows, HDIM))
    results = pl.pallas_call(
        pair_kernel,
        out_shape=(low((rows, width)), high((rows, width)), low((rows, width)), high((rows, HDIM))),
        in_specs=[hbm] * 7,
        out_specs=(vmem,) * 4,
        scratch_shapes=[
            low((branches, rows, width)),
            low((branches, rows, width)),
            low((branches, 2 * rows, width)),
            low((branches, 2 * rows, width)),
            high((branches, rows, width)),
            by_head,
            by_head,
            by_head,
            by_head,
            low((rows, width)),
            low((rows, width)),
            stats,
            stats,
            low((groups, TILE, HDIM)),
            low((groups, TILE, HDIM)),
            high((rows, HDIM)),
            high((rows, HDIM)),
            low((1, width)),
            pltpu.VMEM((1, 1), jnp.int32),
            pltpu.VMEM((1, 1), jnp.int32),
            high((1, width)),
            high((1, width)),
            high((1, width)),
            high((1, width)),
            dma((7,)),
            dma((2, 2 * groups)),
            dma((2, groups)),
            dma((2, groups)),
            dma((2, pieces)),
            dma((2, groups)),
            dma((2, pieces)),
            dma((2, 2)),
            pltpu.SemaphoreType.REGULAR((3,)),
        ],
        compiler_params=pltpu.CompilerParams(collective_id=0, has_side_effects=True),
    )(
        queries[0, 0], keys[0, 0], values[0, 0], latents[0, 0], gain, steps_table,
        flags.reshape(1, 1),
    )
    whole = jax.ShapeDtypeStruct((rows, width), jnp.bfloat16)
    denoised, next_latents = pl.pallas_call(
        place_kernel,
        out_shape=(whole, whole),
        in_specs=[vmem] * 4,
        out_specs=(hbm, hbm),
        scratch_shapes=[low((rows, width)), dma((groups + 1,))],
    )(*(pltpu.with_memory_space_constraint(part, pltpu.VMEM) for part in results))
    return (denoised[None, None], next_latents[None, None])


def per_device(*blocks):
    branches, rows, width = blocks[0].shape[2:]
    paired = (
        lax.axis_size("seq") == 2 * 2
        and lax.axis_size("expert") == 2
        and branches == 2
        and rows % (2 * TILE) == 0
        and rows // TILE * HEADS_AT_ONCE * branches <= HDIM
        and HEADS_AT_ONCE * branches <= TILE
        and width % (HEADS_AT_ONCE * HDIM) == 0
        and width // (HEADS_AT_ONCE * HDIM) > MEET
    )
    return (exchange_queries if paired else exchange_heads)(*blocks)


def solution(mesh):
    placed = (
        P("expert", "batch", None, "seq", None),
        P("expert", "batch", None, "seq", None),
        P("expert", "batch", None, "seq", None),
        P("expert", "batch", "seq", None),
        P("expert", None),
        P("expert", "batch"),
        P("batch"),
    )
    return jax.shard_map(
        per_device,
        mesh=mesh,
        in_specs=placed,
        out_specs=(P("expert", "batch", "seq", None), P("expert", "batch", "seq", None)),
        check_vma=False,
    )
```
